256 devices in a mesh: lvl: 4 (over y), gz: 32 (over z_hi, x, core), gy: 2 (over z_lo).
Axes of the slice: x: 4, y: 4, z: 8 (z_hi: 4, z_lo: 2; z = z_hi * 2 + z_lo), core: 2. Of those that a mesh axis runs over, the one named last changes fastest.
Arguments:
- fine_field: float32 [256, 512, 1024], P('gz', 'gy', 'lvl'), may hold values from -1.2 to 1.2
- noise_pair: float32 [2, 256, 512, 1024], P(None, 'gz', 'gy', 'lvl'), may hold values from -4 to 4
Outputs:
- fine_next: float32 [256, 512, 1024], P('gz', 'gy', 'lvl')
- correction: float32 [128, 256, 512], P('gz', 'gy', 'lvl')
The draws below stay inside these ranges and needn't reach their ends.
All inputs are finite; a program needn't handle non-finite values.
Results may differ from the reference program's by a relative error of at most 0.00014.
Values sent between devices are 32-bit elements; how exact they have to be, the bound alone decides.
No kernel may reach another device: no remote copies, remote signals or barrier semaphores. Data moves between devices by JAX's collectives and lax.ppermute only.
A program may use at most 64 MiB of HBM per device.

```python
import jax
import jax.numpy as jnp

NX = 256
NY = 512
NZ = 1024


def block_scale(rng, extent, cuts, least, largest):
    def one(axis_at, shards_of):
        draws = jax.random.uniform(jax.random.fold_in(jax.random.fold_in(rng, 6), axis_at), (shards_of,), jnp.float32, least / len(cuts), largest / len(cuts))
        return jnp.repeat(jnp.exp(draws), extent[axis_at] // shards_of).reshape((-1,) + (1,) * (len(extent) - axis_at - 1))

    level = one(*cuts[0])
    for cut in cuts[1:]:
        level = level * one(*cut)
    return level


def scatter_about(stream_key, extent, deviation, bound, pieces=(), dtype=jnp.bfloat16):
    values = jax.random.normal(stream_key, extent, jnp.float32) * deviation
    if len(pieces) > 0:
        values = block_scale(stream_key, extent, pieces, -0.22, 0.18) * values
    return jnp.clip(values, min=-bound, max=bound).astype(dtype)


def setup_inputs(seed: int = 0) -> dict:
    streams_of = jax.random.split(jax.random.key(seed), 3)
    return {
        "fine_field": jnp.clip(jax.random.uniform(streams_of[0], (NX, NY, NZ), jnp.float32, -1.2, 1.2) * block_scale(streams_of[0], (NX, NY, NZ), ((0, 32), (1, 2), (2, 4)), -0.4, 0.0), -1.2, 1.2),
        "noise_pair": scatter_about(streams_of[1], (2, NX, NY, NZ), 1.0, 4.0, ((1, 32), (2, 2), (3, 4)), jnp.float32),
    }


noise_amp = 0.3


def advance(field, forcing, spread, react):
    beside = jnp.roll(field, 1, 0) + jnp.roll(field, -1, 0)
    beside = beside + jnp.roll(field, 1, 1) + jnp.roll(field, -1, 1)
    beside = beside + jnp.roll(field, 1, 2) + jnp.roll(field, -1, 2)
    return field + spread * (beside - 6.0 * field) + react * (field - field * field * field) + noise_amp * forcing


def coarsen(values):
    first, second, third = values.shape
    blocks = values.reshape(first // 2, 2, second // 2, 2, third // 2, 2)
    return blocks.sum(axis=(1, 3, 5)) * 0.125


def reference(fine_field, noise_pair):
    middle = advance(fine_field, noise_pair[0], 0.15, 0.1)
    fine_next = advance(middle, noise_pair[1], 0.15, 0.1)
    coarse_start = coarsen(fine_field)
    coarse_noise = coarsen(noise_pair[0] + noise_pair[1])
    coarse_next = advance(coarse_start, coarse_noise, 0.075, 0.2)
    return fine_next, coarsen(fine_next) - coarse_next
```

```python
import jax
import jax.numpy as jnp
from jax import lax
from jax.experimental import pallas as pl
from jax.experimental.pallas import tpu as pltpu
from jax.sharding import PartitionSpec as P

F32 = jnp.float32
noise_amp = 0.3
NXB, NYB, NZB = 8, 256, 256
LANES = 128
TOP = 8
PADDED = NYB + 2 * TOP
CHUNK = 64

vmem = pl.BlockSpec(memory_space=pltpu.VMEM)
hbm = pl.BlockSpec(memory_space=pl.ANY)


def lane_iota(rows=CHUNK):
    return lax.broadcasted_iota(jnp.int32, (rows, LANES), 1)


def row_iota(rows=CHUNK):
    return lax.broadcasted_iota(jnp.int32, (rows, LANES), 0)


def pair_table():
    source = lax.broadcasted_iota(jnp.int32, (NZB, LANES), 0) >> 1
    target = lax.broadcasted_iota(jnp.int32, (NZB, LANES), 1)
    return jnp.where(source == target, 1.0, 0.0).astype(jnp.bfloat16)


def pair_lanes(values, table):
    first = values.astype(jnp.bfloat16)
    rest = values - first.astype(F32)
    second = rest.astype(jnp.bfloat16)
    third = (rest - second.astype(F32)).astype(jnp.bfloat16)
    total = jnp.dot(third, table, preferred_element_type=F32)
    total = total + jnp.dot(second, table, preferred_element_type=F32)
    return total + jnp.dot(first, table, preferred_element_type=F32)


def pair_rows(ref, half):
    even = ref[half, pl.ds(0, NYB // 2, stride=2), :]
    odd = ref[half, pl.ds(1, NYB // 2, stride=2), :]
    return even + odd


def pair_both(ref, table):
    return pair_lanes(jnp.concatenate([pair_rows(ref, 0), pair_rows(ref, 1)], axis=1), table)


def beside_lanes(left, right, low, high, lane):
    left_up, left_down = pltpu.roll(left, 1, 1), pltpu.roll(left, LANES - 1, 1)
    right_up, right_down = pltpu.roll(right, 1, 1), pltpu.roll(right, LANES - 1, 1)
    first, last = lane == 0, lane == LANES - 1
    return (
        jnp.where(first, low, left_up) + jnp.where(last, right_down, left_down),
        jnp.where(first, left_up, right_up) + jnp.where(last, high, right_down),
    )


def react(v):
    return v * (0.2 - 0.1 * (v * v))


def parity():
    return lax.rem(lax.axis_index("gz"), 2)


def rows_to_lanes(ref, scratch):
    scratch[0:16, :] = ref[...]
    return [scratch[:, k * LANES : (k + 1) * LANES].T for k in range(2)]


def lanes_to_rows(ref, tiles):
    for k in range(2):
        ref[:, k * LANES : (k + 1) * LANES] = tiles[k].T[0:16]


def start_all(copies):
    for copy in copies:
        copy.start()


def wait_all(copies):
    for copy in copies:
        copy.wait()


def half(k):
    return pl.ds(k * LANES, LANES)


def faces_kernel(u, noise, bp, al, zlo, zhi, yf, planes, forcing, pairs, sems):
    par = parity()
    outer = (par * 7, 7 - par * 7)
    inner = (1 + par * 5, 6 - par * 5)
    spans = ((0, 2), (6, 2), (2, 4))
    field = [
        [
            pltpu.make_async_copy(
                u.at[pl.ds(at, n), :, half(k)], planes.at[pl.ds(at, n), k, pl.ds(TOP, NYB), :], sems.at[2 * i + k]
            )
            for k in range(2)
        ]
        for i, (at, n) in enumerate(spans)
    ]
    force = [
        pltpu.make_async_copy(noise.at[0, 7 * i, :, half(k)], forcing.at[i, k], sems.at[6 + 2 * i + k])
        for i in range(2)
        for k in range(2)
    ]
    start_all(field[0] + field[1] + force + field[2])
    zero = jnp.zeros((8, LANES), F32)
    for x in (0, 7):
        for k in range(2):
            planes[x, k, 0:TOP, :] = zero
            planes[x, k, TOP + NYB :, :] = zero
    table = pair_table()
    lane = lane_iota()
    wait_all(field[0] + field[1] + force)
    for side, (ref, at) in enumerate(((bp, 0), (al, NYB))):
        x, xi = outer[side], inner[side]
        fi = par if side == 0 else 1 - par
        for r in range(0, NYB, CHUNK):
            v = [planes[x, k, TOP + r : TOP + r + CHUNK, :] for k in range(2)]
            z = beside_lanes(v[0], v[1], 0.0, 0.0, lane)
            for k in range(2):
                within = planes[xi, k, TOP + r : TOP + r + CHUNK, :]
                beside = (
                    z[k]
                    + planes[x, k, TOP - 1 + r : TOP - 1 + r + CHUNK, :]
                    + planes[x, k, TOP + 1 + r : TOP + 1 + r + CHUNK, :]
                    + within
                )
                ref[at + r : at + r + CHUNK, half(k)] = (
                    react(v[k]) + 0.15 * beside + noise_amp * forcing[fi, k, r : r + CHUNK, :]
                )
                pairs[k, r : r + CHUNK, :] = v[k] + within
                if side == 1:
                    al[r : r + CHUNK, half(k)] = v[k]
        coarse = pair_both(pairs, table)
        for k in range(2):
            ref[at + NYB : at + NYB + 64, half(k)] = coarse[64 * k : 64 * k + 64]
    wait_all(field[2])
    for x in range(NXB):
        for k in range(2):
            for n, row in enumerate((0, 1, NYB - 1, NYB - 2)):
                yf[8 * n + x : 8 * n + x + 1, half(k)] = planes[x, k, TOP + row : TOP + row + 1, :]
    for k, ref in ((0, zlo), (1, zhi)):
        tiles = []
        for r in range(0, NYB, LANES):
            wide = lane_iota(LANES)
            tile = planes[0, k, TOP + r : TOP + r + LANES, :]
            tile = pltpu.roll(tile, 2, 1) if k else tile
            for x in range(1, NXB):
                moved = pltpu.roll(planes[x, k, TOP + r : TOP + r + LANES, :], 2 * x + 2 * k, 1)
                tile = jnp.where(wide >= 2 * x, moved, tile)
            tiles.append(tile)
        lanes_to_rows(ref, tiles)


def faces(u, noise):
    return pl.pallas_call(
        faces_kernel,
        out_shape=(
            jax.ShapeDtypeStruct((NYB + 64, NZB), F32),
            jax.ShapeDtypeStruct((2 * NYB + 64, NZB), F32),
            jax.ShapeDtypeStruct((16, NYB), F32),
            jax.ShapeDtypeStruct((16, NYB), F32),
            jax.ShapeDtypeStruct((32, NZB), F32),
        ),
        in_specs=[hbm, hbm],
        out_specs=(vmem,) * 5,
        scratch_shapes=[
            pltpu.VMEM((NXB, 2, PADDED, LANES), F32),
            pltpu.VMEM((2, 2, NYB, LANES), F32),
            pltpu.VMEM((2, NYB, LANES), F32),
            pltpu.SemaphoreType.DMA((10,)),
        ],
        name="faces",
    )(u, noise)


def middle_kernel(u, noise, ab, al, glo, ghi, gy, mp, mzlo, mzhi, my, planes, forcing, rows, sems):
    par = parity()
    field = [
        pltpu.make_async_copy(
            u.at[pl.ds(2 * i, 2), :, half(k)], planes.at[pl.ds(2 * i + 1, 2), k, pl.ds(TOP, NYB), :], sems.at[0, 2 * i + k]
        )
        for i in range(4)
        for k in range(2)
    ]
    force = [
        pltpu.make_async_copy(
            noise.at[0, pl.ds(2 * i, 2), :, half(k)], forcing.at[pl.ds(2 * i, 2), k], sems.at[1, 2 * i + k]
        )
        for i in range(4)
        for k in range(2)
    ]
    for i in range(8):
        field[i].start()
        force[i].start()
    for k in range(2):
        planes[par * 9, k, TOP : TOP + NYB, :] = ab[:, half(k)]
        planes[9 - par * 9, k, TOP : TOP + NYB, :] = al[0:NYB, half(k)]
        for x in range(NXB):
            planes[x + 1, k, TOP - 1 : TOP, :] = gy[16 + x : 17 + x, half(k)]
            planes[x + 1, k, TOP + NYB : TOP + NYB + 1, :] = gy[x : x + 1, half(k)]
    low = rows_to_lanes(glo, rows)
    high = rows_to_lanes(ghi, rows)
    lane = lane_iota()
    wait_all(field[0:4] + force[0:2])
    for x in range(NXB):
        if x % 2 == 0 and x > 0:
            wait_all(force[x : x + 2])
            if x < 6:
                wait_all(field[x + 2 : x + 4])
        for r in range(0, NYB, CHUNK):
            at, tile = r % LANES, r // LANES
            v = [planes[x + 1, k, TOP + r : TOP + r + CHUNK, :] for k in range(2)]
            z = beside_lanes(
                v[0],
                v[1],
                pltpu.roll(low[tile][at : at + CHUNK], LANES - (2 * x + 1), 1),
                pltpu.roll(high[tile][at : at + CHUNK], LANES - 1 - 2 * x, 1),
                lane,
            )
            for k in range(2):
                beside = (
                    z[k]
                    + planes[x + 1, k, TOP - 1 + r : TOP - 1 + r + CHUNK, :]
                    + planes[x + 1, k, TOP + 1 + r : TOP + 1 + r + CHUNK, :]
                    + planes[x, k, TOP + r : TOP + r + CHUNK, :]
                    + planes[x + 2, k, TOP + r : TOP + r + CHUNK, :]
                )
                mp[x, k, TOP + r : TOP + r + CHUNK, :] = (
                    react(v[k]) + 0.15 * beside + noise_amp * forcing[x, k, r : r + CHUNK, :]
                )
    for k in range(2):
        for n, row in enumerate((0, NYB - 1)):
            at = TOP + row
            for x in range(NXB):
                my[8 * n + x : 8 * n + x + 1, half(k)] = mp[x, k, at : at + 1, :]
            my[16 + 2 * n : 17 + 2 * n, half(k)] = planes[0, k, at : at + 1, :]
            my[17 + 2 * n : 18 + 2 * n, half(k)] = planes[9, k, at : at + 1, :]
    my[20:24, :] = jnp.zeros((4, NZB), F32)
    wide = lane_iota(LANES)
    for k, ref in ((0, mzlo), (1, mzhi)):
        tiles = []
        for r in range(0, NYB, LANES):
            span = slice(TOP + r, TOP + r + LANES)
            columns = [mp[x, k, span, :] for x in range(NXB)] + [planes[0, k, span, :], planes[9, k, span, :]]
            tile = pltpu.roll(columns[0], 1, 1) if k else columns[0]
            for n in range(1, 10):
                tile = jnp.where(wide >= n, pltpu.roll(columns[n], n + k, 1), tile)
            tiles.append(tile)
        lanes_to_rows(ref, tiles)


def middle(u, noise, ab, al, glo, ghi, gy):
    return pl.pallas_call(
        middle_kernel,
        out_shape=(
            jax.ShapeDtypeStruct((NXB, 2, PADDED, LANES), F32),
            jax.ShapeDtypeStruct((16, NYB), F32),
            jax.ShapeDtypeStruct((16, NYB), F32),
            jax.ShapeDtypeStruct((24, NZB), F32),
        ),
        in_specs=[hbm, hbm] + [vmem] * 5,
        out_specs=(vmem,) * 4,
        scratch_shapes=[
            pltpu.VMEM((NXB + 2, 2, PADDED, LANES), F32),
            pltpu.VMEM((NXB, 2, NYB, LANES), F32),
            pltpu.VMEM((LANES, NYB), F32),
            pltpu.SemaphoreType.DMA((2, 8)),
        ],
        name="middle",
    )(u, noise, ab, al, glo, ghi, gy)


def coarse_kernel(u, noise, glo, ghi, gy, cb, planes, forcing, pairs, sums, ghosts, square, sems):
    field = [
        pltpu.make_async_copy(u.at[pl.ds(2 * i, 2), :, half(k)], planes.at[pl.ds(2 * i, 2), k], sems.at[0, 2 * i + k])
        for i in range(4)
        for k in range(2)
    ]
    force = [
        pltpu.make_async_copy(
            noise.at[0, pl.ds(2 * i, 2), :, half(k)], forcing.at[pl.ds(2 * i, 2), k], sems.at[1, 2 * i + k]
        )
        for i in range(4)
        for k in range(2)
    ]
    start_all(field + force)
    table = pair_table()
    for n, ref in enumerate((glo, ghi)):
        for i in range(4):
            ghosts[8 * n + i : 8 * n + i + 1, :] = (
                ref[4 * i : 4 * i + 1, :] + ref[4 * i + 1 : 4 * i + 2, :] + ref[4 * i + 2 : 4 * i + 3, :] + ref[4 * i + 3 : 4 * i + 4, :]
            )
            at = 16 * (1 - n) + 2 * i
            ghosts[8 * n + 4 + i : 8 * n + 5 + i, :] = (
                gy[at : at + 1, :] + gy[at + 1 : at + 2, :] + gy[at + 8 : at + 9, :] + gy[at + 9 : at + 10, :]
            )
    paired = pair_lanes(ghosts[...], table)
    square[0:16, :] = paired
    for i in range(4):
        sums[i, TOP - 1 : TOP, :] = paired[4 + i : 5 + i]
        sums[i, TOP + LANES : TOP + LANES + 1, :] = paired[12 + i : 13 + i]
    column = square[...].T
    for i in range(4):
        wait_all(field[2 * i : 2 * i + 2])
        for k in range(2):
            pairs[k] = planes[2 * i, k] + planes[2 * i + 1, k]
        sums[i, TOP : TOP + LANES, :] = pair_both(pairs, table)
    lane = lane_iota(LANES)
    for i in range(4):
        wait_all(force[2 * i : 2 * i + 2])
        for k in range(2):
            pairs[k] = forcing[2 * i, k] + forcing[2 * i + 1, k]
        drive = pair_both(pairs, table)
        v = sums[i, TOP : TOP + LANES, :]
        low = pltpu.roll(column, LANES - i, 1) if i else column
        high = pltpu.roll(column, LANES - 1 - (8 + i), 1)
        beside = jnp.where(lane == 0, low, pltpu.roll(v, 1, 1)) + jnp.where(
            lane == LANES - 1, high, pltpu.roll(v, LANES - 1, 1)
        )
        beside = beside + sums[i, TOP - 1 : TOP - 1 + LANES, :] + sums[i, TOP + 1 : TOP + 1 + LANES, :]
        if i > 0:
            beside = beside + sums[i - 1, TOP : TOP + LANES, :]
        if i < 3:
            beside = beside + sums[i + 1, TOP : TOP + LANES, :]
        c = 0.125 * v
        cb[i] = c * (0.2 * (c * c) - 0.75) - (0.075 * 0.125) * beside - (noise_amp * 0.125) * drive


def coarse(u, noise, glo, ghi, gy):
    return pl.pallas_call(
        coarse_kernel,
        out_shape=jax.ShapeDtypeStruct((4, LANES, LANES), F32),
        in_specs=[hbm, hbm] + [vmem] * 3,
        out_specs=vmem,
        scratch_shapes=[
            pltpu.VMEM((NXB, 2, NYB, LANES), F32),
            pltpu.VMEM((NXB, 2, NYB, LANES), F32),
            pltpu.VMEM((2, NYB, LANES), F32),
            pltpu.VMEM((4, LANES + 2 * TOP, LANES), F32),
            pltpu.VMEM((16, NYB), F32),
            pltpu.VMEM((LANES, LANES), F32),
            pltpu.SemaphoreType.DMA((2, 8)),
        ],
        name="coarse",
    )(u, noise, glo, ghi, gy)


def final_kernel(
    u, noise, mp, bp, al, glo, ghi, gy, cb, fine, corr, edges, forcing, ghost, result, pairs, rows, sems, done
):
    par = parity()
    rim = [
        pltpu.make_async_copy(u.at[7 * i, :, half(k)], edges.at[i, k], sems.at[2 * i + k])
        for i in range(2)
        for k in range(2)
    ]
    force = [
        pltpu.make_async_copy(
            noise.at[1, pl.ds(2 * i, 2), :, half(k)], forcing.at[pl.ds(2 * i, 2), k], sems.at[4 + 2 * i + k]
        )
        for i in range(4)
        for k in range(2)
    ]
    start_all(rim + force)
    low = rows_to_lanes(glo, rows)
    high = rows_to_lanes(ghi, rows)
    lane, row = lane_iota(), row_iota()
    table = pair_table()
    first, last = row == 0, row == CHUNK - 1
    wait_all(rim)
    for side, (ref, at) in enumerate(((bp, 0), (al, NYB))):
        i = par if side == 0 else 1 - par
        for r in range(0, NYB, CHUNK):
            tile, span = r // LANES, slice(r % LANES, r % LANES + CHUNK)
            for k in range(2):
                extra = edges[i, k, r : r + CHUNK, :]
                if r == 0:
                    extra = extra + jnp.where(first, jnp.where(i == 0, gy[18:19, half(k)], gy[19:20, half(k)]), 0.0)
                if r == NYB - CHUNK:
                    extra = extra + jnp.where(last, jnp.where(i == 0, gy[16:17, half(k)], gy[17:18, half(k)]), 0.0)
                if k == 0:
                    extra = extra + jnp.where(lane == 0, pltpu.roll(low[tile][span], LANES - 8 - i, 1), 0.0)
                else:
                    extra = extra + jnp.where(lane == LANES - 1, pltpu.roll(high[tile][span], LANES - 1 - 8 - i, 1), 0.0)
                ghost[i, k, r : r + CHUNK, :] = ref[at + r : at + r + CHUNK, half(k)] + 0.15 * extra
    outs = []
    for x in range(NXB):
        if x % 2 == 0:
            wait_all(force[x : x + 2])
        for r in range(0, NYB, CHUNK):
            tile, span = r // LANES, slice(r % LANES, r % LANES + CHUNK)
            v = [mp[x, k, TOP + r : TOP + r + CHUNK, :] for k in range(2)]
            z = beside_lanes(
                v[0],
                v[1],
                pltpu.roll(low[tile][span], LANES - x, 1) if x else low[tile][span],
                pltpu.roll(high[tile][span], LANES - 1 - x, 1),
                lane,
            )
            for k in range(2):
                up = mp[x, k, TOP - 1 + r : TOP - 1 + r + CHUNK, :]
                down = mp[x, k, TOP + 1 + r : TOP + 1 + r + CHUNK, :]
                if r == 0:
                    up = jnp.where(first, gy[8 + x : 9 + x, half(k)], up)
                if r == NYB - CHUNK:
                    down = jnp.where(last, gy[x : x + 1, half(k)], down)
                below = mp[x - 1, k, TOP + r : TOP + r + CHUNK, :] if x > 0 else ghost[0, k, r : r + CHUNK, :]
                above = mp[x + 1, k, TOP + r : TOP + r + CHUNK, :] if x < 7 else ghost[1, k, r : r + CHUNK, :]
                value = react(v[k]) + 0.15 * (z[k] + up + down + below + above)
                result[x, k, r : r + CHUNK, :] = value + noise_amp * forcing[x, k, r : r + CHUNK, :]
                if x % 2 == 0:
                    pairs[k, r : r + CHUNK, :] = value
                else:
                    pairs[k, r : r + CHUNK, :] += value
        for k in range(2):
            out = pltpu.make_async_copy(result.at[x, k], fine.at[x, :, half(k)], done.at[2 * x + k])
            out.start()
            outs.append(out)
        if x % 2 == 1:
            i = x // 2
            total = 0.125 * pair_both(pairs, table) + cb[i]
            if i in (0, 3):
                side_b, side_a = bp[NYB : NYB + 64, :], al[2 * NYB : 2 * NYB + 64, :]
                far = jnp.where(par == (0 if i == 0 else 1), side_b, side_a)
                total = total - (0.075 * 0.125) * jnp.concatenate([far[:, 0:LANES], far[:, LANES:]], axis=0)
            corr[i] = total
    wait_all(outs)


def final(u, noise, mp, bp, al, glo, ghi, gy, cb):
    return pl.pallas_call(
        final_kernel,
        out_shape=(
            jax.ShapeDtypeStruct((NXB, NYB, NZB), F32),
            jax.ShapeDtypeStruct((4, LANES, LANES), F32),
        ),
        in_specs=[hbm, hbm] + [vmem] * 7,
        out_specs=(hbm, vmem),
        scratch_shapes=[
            pltpu.VMEM((2, 2, NYB, LANES), F32),
            pltpu.VMEM((NXB, 2, NYB, LANES), F32),
            pltpu.VMEM((2, 2, NYB, LANES), F32),
            pltpu.VMEM((NXB, 2, NYB, LANES), F32),
            pltpu.VMEM((2, NYB, LANES), F32),
            pltpu.VMEM((LANES, NYB), F32),
            pltpu.SemaphoreType.DMA((12,)),
            pltpu.SemaphoreType.DMA((16,)),
        ],
        name="final",
    )(u, noise, mp, bp, al, glo, ghi, gy, cb)


def swap_pairs(values, axis, first):
    count = lax.axis_size(axis)
    pairs = []
    for i in range(first, count, 2):
        j = (i + 1) % count
        pairs += [(i, j), (j, i)]
    return lax.ppermute(values, axis, pairs)


def shift(values, axis, by):
    count = lax.axis_size(axis)
    return lax.ppermute(values, axis, [(i, (i + by) % count) for i in range(count)])


def on_device(u, noise):
    par = lax.axis_index("gz") % 2
    ab = lax.dynamic_slice_in_dim(u, par * 7, 1, axis=0).reshape(NYB, NZB)
    far_ab = swap_pairs(ab, "gz", 1)
    bp, al, zlo, zhi, yf = faces(u, noise)
    far_bp = swap_pairs(bp, "gz", 1)
    far_al = swap_pairs(al, "gz", 0)
    glo = shift(zhi, "lvl", 1)
    ghi = shift(zlo, "lvl", -1)
    gy = swap_pairs(yf, "gy", 0)
    mp, mzlo, mzhi, my = middle(u, noise, far_ab, far_al, glo, ghi, gy)
    mlo = shift(mzhi, "lvl", 1)
    mhi = shift(mzlo, "lvl", -1)
    mgy = swap_pairs(my, "gy", 0)
    cb = coarse(u, noise, glo, ghi, gy)
    return final(u, noise, mp, far_bp, far_al, mlo, mhi, mgy, cb)


def solution(mesh):
    in_specs = (P("gz", "gy", "lvl"), P(None, "gz", "gy", "lvl"))
    out_specs = (P("gz", "gy", "lvl"), P("gz", "gy", "lvl"))
    return jax.shard_map(on_device, mesh=mesh, in_specs=in_specs, out_specs=out_specs, check_vma=False)
```
